32 devices in a mesh: section: 4 (over y, x), node: 4 (over z), torus: 2 (over core).
Axes of the slice: x: 2, y: 2, z: 4, core: 2. Of those that a mesh axis runs over, the one named last changes fastest.
Arguments:
- act_in: bfloat16 [4, 1024, 7168], P('section', 'node', 'torus'), may hold values from -28 to 28
- next_in: bfloat16 [1024, 7168], P('node', 'torus'), may hold values from -42 to 42
- routes: int32 [2, 4, 1024, 2], P(None, 'section', 'node'), may hold values from 0 to 3, all different within a row; in each aligned block of 256 rows (0 to 255, 256 to 511, ..., all dimensions but the last counted through in order) at most 160 rows name the same one
- route_w: float32 [2, 4, 1024, 2], P(None, 'section', 'node'), may hold values from 0.2 to 1
- hist: float32 [4], P('section'), may hold values from 2 to 8
- gate_w: bfloat16 [4, 4, 7168, 1024], P('section', 'node', 'torus'), may hold values from -0.0625 to 0.0625
- up_w: bfloat16 [4, 4, 7168, 1024], P('section', 'node', 'torus'), may hold values from -0.0625 to 0.0625
- down_w: bfloat16 [4, 4, 1024, 7168], P('section', 'node', None, 'torus'), may hold values from -0.09375 to 0.09375
Outputs:
- act_out: bfloat16 [2, 4, 1024, 7168], P(None, 'section', 'node', 'torus')
- peak_out: float32 [4, 2], P('section')
The draws below stay inside these ranges and needn't reach their ends.
Inputs may be any that keep to these rules, and one draw needn't show every extreme that they name: `routes`: each token names 2 different experts; within the 256 tokens of one index of node (aligned blocks of rows of one tick and layer) no expert is named more than 160 times, a bound that some block reaches.
All inputs are finite; a program needn't handle non-finite values.
Results may differ from the reference program's by a relative error of at most 0.012.
Values may be sent and summed in bfloat16 or wider, within the bound.
A program may use at most 128 MiB of HBM per device.

```python
import math
import jax
import jax.numpy as jnp
import numpy as np
from jax import lax

D = 7168
FFW = 1024
TOPK = 2
TICKS = 2
TOK_DEV = 256
SECTIONS = 4
EXPERTS = 4
CAP = 160
TOKENS = 1024
N_NODE = 4


def rising_rows(key, array_shape, factor):
    noise_key, scale_key = jax.random.split(key)
    rising = 1.0 + 2.0 * jnp.arange(TOKENS, dtype=jnp.float32) / TOKENS
    noise = jnp.clip(jax.random.normal(noise_key, array_shape, jnp.float32), -6.0, 6.0)
    spread = jnp.exp(jax.random.uniform(scale_key, array_shape[:-1] + (1,), jnp.float32, -0.7, 0.4))
    return (noise * spread * rising[:, None] * factor).astype(jnp.bfloat16)


def draw_act_in(key, part):
    return rising_rows(jax.random.fold_in(key, 11), (SECTIONS, TOKENS, D), 1.0)


def draw_next_in(key, part):
    return rising_rows(jax.random.fold_in(key, 23), (TOKENS, D), 1.5)


def levels(stream_key, dims, shards, low, top_value):
    level, own = 1.0, jax.random.fold_in(stream_key, 6)
    for axis_at, blocks in shards:
        steps = jnp.exp(jax.random.uniform(jax.random.fold_in(own, axis_at), (blocks,), jnp.float32, low / len(shards), top_value / len(shards)))
        level = level * jnp.repeat(steps, dims[axis_at] // blocks).reshape([-1 if axis == axis_at else 1 for axis in range(len(dims))])
    return level


def routed_block(own_key, own, number, rows, amount, top, reach, lean):
    order = jax.random.permutation(own_key, amount)
    heavy_load, ordinary = shares(amount, rows * top, reach, lean, True), shares(amount, rows * top, reach, lean, False)
    places = jnp.arange(amount)

    def named(tallies, turn):
        used = int((tallies > 0).sum())
        fixed = max(1, used // 4)
        shifted = fixed + (places - fixed + turn * (used - fixed)) % max(1, amount - fixed)
        return jnp.zeros((amount,), jnp.int32).at[order[jnp.where(places < fixed, places, shifted)]].set(jnp.asarray(tallies, jnp.int32))

    tallies = jnp.where(number % 4 == 0, named(heavy_load, number // 4), named(ordinary, number - number // 4 - 1))
    mixed = jax.random.permutation(jax.random.fold_in(own, 3), amount)
    source_of, sink = mixed[0:amount // 2 * 2:2], mixed[1:amount // 2 * 2:2]
    slack = jnp.minimum(tallies[source_of] - 1, reach - tallies[sink]) // 2
    slack = jnp.where((source_of == order[0]) | (sink == order[0]) | (tallies[sink] == 0), 0, jnp.maximum(slack, 0))
    shifted = jax.random.randint(jax.random.fold_in(own, 4), (amount // 2,), 0, 1 << 20) % (slack + 1)
    tallies = tallies.at[source_of].add(-shifted).at[sink].add(shifted)
    members = jnp.searchsorted(jnp.cumsum(tallies), jnp.arange(rows * top), side="right").astype(jnp.int32)
    grid = members.reshape(top, rows).T
    grid = grid[jax.random.permutation(jax.random.fold_in(own, 1), rows)]
    turn = jax.random.randint(jax.random.fold_in(own, 2), (rows, 1), 0, top)
    return jnp.take_along_axis(grid, (jnp.arange(top)[None, :] + turn) % top, axis=1)


def shares(count, total, limit, lean, full):
    portions = [(1 << 20) // math.isqrt(rank ** lean) + 1 for rank in range(1, count + 1)]
    largest = limit if full else min(limit, max(-(-total // count), total * portions[0] // sum(portions)))
    least = 1 if total - largest >= count - 1 else 0
    given, surplus = [largest] + [least] * (count - 1), total - largest - least * (count - 1)
    while surplus > 0:
        free = [i for i in range(1, count) if given[i] < largest] or [i for i in range(1, count) if given[i] < limit]
        pool, remaining = sum([portions[i] for i in free]), surplus
        for i in free:
            more = min(limit - given[i], max(1, remaining * portions[i] // pool), surplus)
            given[i] = given[i] + more
            surplus = surplus - more
    return np.array(given)


def bell_draw(stream_key, extent, scale, reach, cuts=(), held_as=jnp.bfloat16):
    values = scale * jax.random.normal(stream_key, extent, jnp.float32)
    if cuts:
        values = values * levels(stream_key, extent, cuts, -0.22, 0.18)
    return jnp.clip(values, -reach, reach).astype(held_as)


def setup_inputs(seed: int = 0) -> dict:
    key_of = jax.random.split(jax.random.key(seed), 9)
    act_in = draw_act_in(jax.random.fold_in(key_of[8], 71), 0)
    next_in = draw_next_in(jax.random.fold_in(key_of[8], 71), 0)
    routes_keys = jax.random.split(jax.random.fold_in(key_of[2], 1), TICKS * SECTIONS * TOKENS // TOK_DEV)
    routes_turns = jax.random.permutation(jax.random.fold_in(key_of[2], 3), TICKS * SECTIONS * TOKENS // TOK_DEV)
    routes = jax.vmap(lambda own, number: routed_block(jax.random.fold_in(key_of[2], 2), own, number, TOK_DEV, EXPERTS, TOPK, CAP, 2))(routes_keys, routes_turns).reshape((TICKS, SECTIONS, TOKENS, TOPK))
    route_w = jnp.clip(0.2 + 0.8 * jax.random.uniform(key_of[3], (TICKS, SECTIONS, TOKENS, TOPK), jnp.float32) ** levels(key_of[3], (TICKS, SECTIONS, TOKENS, TOPK), ((1, 4), (2, 4)), -0.2, 0.2), 0.2, 1.0)
    hist = jnp.clip(2.0 + 6.0 * jax.random.uniform(key_of[4], (SECTIONS,), jnp.float32) ** levels(key_of[4], (SECTIONS,), ((0, 4),), -0.2, 0.2), 2.0, 8.0)
    gate_w = bell_draw(key_of[5], (SECTIONS, EXPERTS, D, FFW), D ** -0.5, 0.0625, ((0, 4), (1, 4), (2, 2)))
    up_w = bell_draw(key_of[6], (SECTIONS, EXPERTS, D, FFW), D ** -0.5, 0.0625, ((0, 4), (1, 4), (2, 2)))
    down_w = bell_draw(key_of[7], (SECTIONS, EXPERTS, FFW, D), (4 * FFW) ** -0.5, 0.09375, ((0, 4), (1, 4), (3, 2)))
    return dict(act_in=act_in, next_in=next_in, routes=routes, route_w=route_w, hist=hist, gate_w=gate_w, up_w=up_w, down_w=down_w)


FP8_LIMIT = 448.0


def expert_rows(token_rows, gate_mat, up_mat, down_mat, dequant):
    gate_val = jnp.dot(token_rows, gate_mat, preferred_element_type=jnp.float32) * dequant
    up_val = jnp.dot(token_rows, up_mat, preferred_element_type=jnp.float32) * dequant
    hidden = (jax.nn.silu(gate_val) * up_val).astype(jnp.bfloat16)
    return jnp.dot(hidden, down_mat, preferred_element_type=jnp.float32).astype(jnp.bfloat16)


def moe_layer(stream, quant_scale, expert_of, weight_of, gate_all, up_all, down_all):
    quantized = jnp.clip(stream.astype(jnp.float32) * (FP8_LIMIT / quant_scale), -FP8_LIMIT, FP8_LIMIT).astype(jnp.bfloat16)
    dequant = quant_scale / FP8_LIMIT
    pair_count = TOKENS * TOPK
    flat_expert = expert_of.reshape(pair_count).astype(jnp.int32)
    flat_weight = weight_of.reshape(pair_count)
    slot_total = N_NODE * CAP
    positions = jnp.arange(pair_count, dtype=jnp.int32)

    def per_expert(expert_id):
        sort_keys = jnp.where(flat_expert == expert_id, positions, pair_count)
        chosen = jnp.argsort(sort_keys, stable=True)[:slot_total].astype(jnp.int32)
        is_valid = (flat_expert[chosen] == expert_id).astype(jnp.float32)
        token_ids = chosen // TOPK
        token_rows = quantized[token_ids]
        outputs = expert_rows(token_rows, gate_all[expert_id], up_all[expert_id], down_all[expert_id], dequant)
        return token_ids, outputs.astype(jnp.float32) * (flat_weight[chosen] * is_valid)[:, None]

    token_ids, contrib = lax.map(per_expert, jnp.arange(EXPERTS, dtype=jnp.int32))
    branch = jnp.zeros((TOKENS, D), jnp.float32).at[token_ids.reshape(-1)].add(contrib.reshape(-1, D))
    return (stream.astype(jnp.float32) + branch).astype(jnp.bfloat16)


def reference(act_in, next_in, routes, route_w, hist, gate_w, up_w, down_w):
    first_peaks = []
    first_tick = []
    for section_id in range(SECTIONS):
        stream = act_in[section_id]
        first_peaks.append(jnp.max(jnp.abs(stream.astype(jnp.float32))))
        first_tick.append(moe_layer(stream, hist[section_id], routes[0, section_id], route_w[0, section_id], gate_w[section_id], up_w[section_id], down_w[section_id]))
    second_peaks = []
    second_tick = []
    for section_id in range(SECTIONS):
        stream = next_in if section_id == 0 else first_tick[section_id - 1]
        second_peaks.append(jnp.max(jnp.abs(stream.astype(jnp.float32))))
        second_tick.append(moe_layer(stream, first_peaks[section_id], routes[1, section_id], route_w[1, section_id], gate_w[section_id], up_w[section_id], down_w[section_id]))
    act_out = jnp.stack([jnp.stack(first_tick), jnp.stack(second_tick)])
    peak_out = jnp.stack([jnp.stack(first_peaks), jnp.stack(second_peaks)], axis=1)
    return act_out, peak_out
```

```python
import jax
import jax.numpy as jnp
from jax import lax
from jax.sharding import PartitionSpec as P

FP8_LIMIT = 448.0
MAX_CHUNKS = 4
DEPTH = 2


def shifted(value, axis, steps):
    count = lax.axis_size(axis)
    return lax.ppermute(value, axis, [(i, (i + steps) % count) for i in range(count)])


def swapped(value, axis):
    count = lax.axis_size(axis)
    return lax.ppermute(value, axis, [(i, i ^ 1) for i in range(count)])


def to_next_section(value):
    count = lax.axis_size("section")
    return lax.ppermute(value, "section", [(i, i + 1) for i in range(count - 1)])


def dot(left, right):
    return lax.dot_general(left, right, (((1,), (0,)), ((), ())), preferred_element_type=jnp.float32)


def torus_sum(value):
    if lax.axis_size("torus") == 2:
        return value + swapped(value.astype(jnp.bfloat16), "torus").astype(jnp.float32)
    return lax.psum(value, "torus")


def after(value, *earlier):
    return lax.optimization_barrier((value, *earlier))[0]


def ring_max(value, axis):
    count = lax.axis_size(axis)
    if count & (count - 1):
        return lax.pmax(value, axis)
    step = 1
    while step < count:
        value = jnp.maximum(value, shifted(value, axis, step))
        step *= 2
    return value


def routing_tables(expert_of, weight_of, capacity, n_node, me):
    tokens = expert_of.shape[0]
    pair = jnp.stack([me, me ^ 1]).astype(jnp.float32)
    named = expert_of[:, None, :] == pair[None, :, None]
    hit = jnp.any(named, axis=2)
    wgt = jnp.sum(jnp.where(named, weight_of[:, None, :], 0.0), axis=2)
    earlier = (jnp.arange(tokens)[:, None] > jnp.arange(tokens)[None, :]).astype(jnp.bfloat16)
    slots = jnp.arange(capacity, dtype=jnp.float32)
    rank = dot(earlier, hit.astype(jnp.bfloat16))
    chosen = (rank[:, :, None] == slots) & hit[:, :, None]
    table = chosen.astype(jnp.bfloat16).reshape(tokens, 2 * capacity)
    combine = jnp.where(chosen, wgt[:, :, None], 0.0).astype(jnp.bfloat16)
    return table.T, combine.reshape(tokens, 2 * capacity)


def shards(act_in, next_in, routes, route_w, hist, gate_w, up_w, down_w):
    tokens = act_in.shape[1]
    ticks = routes.shape[0]
    top = routes.shape[3]
    n_node = lax.axis_size("node")
    groups = n_node // 2
    capacity = 5 * tokens * top // (4 * n_node)
    half = groups * capacity
    gate_mat, up_mat, down_mat = gate_w[0, 0], up_w[0, 0], down_w[0, 0]
    width = gate_mat.shape[0]
    count = max(c for c in range(1, MAX_CHUNKS + 1) if width % (128 * c) == 0)
    size = width // count
    me = lax.axis_index("node")
    section_now = lax.axis_index("section")

    own_peak = jnp.max(jnp.abs(act_in[0])).astype(jnp.float32)
    packed = jnp.concatenate(
        [routes.astype(jnp.float32).reshape(-1), route_w.reshape(-1), jnp.full((128,), own_peak)]
    )
    amount = ticks * tokens * top
    known = [packed] + [shifted(packed, "node", -2 * k) for k in range(1, groups)]
    tables = []
    for tick in range(ticks):
        pairs = []
        for info in known:
            expert_of = info[:amount].reshape(ticks, tokens, top)[tick]
            weight_of = info[amount : 2 * amount].reshape(ticks, tokens, top)[tick]
            pairs.append(routing_tables(expert_of, weight_of, capacity, n_node, me))
        tables.append(tuple(zip(*pairs)))

    cuts = [slice(c * size, (c + 1) * size) for c in range(count)]
    streams = [act_in[0][:, cut] for cut in cuts]
    scale = hist[0]
    first_peak = known[0][-1:]
    for info in known[1:]:
        first_peak = jnp.maximum(first_peak, info[-1:])
    first_peak = ring_max(first_peak, "torus")
    first_peak = jnp.maximum(first_peak, swapped(first_peak, "node"))
    outputs, peaks = [], [first_peak[0]]
    for tick in range(ticks):
        select, combine = tables[tick]
        if tick > 0:
            streams = [
                lax.optimization_barrier(
                    jnp.where(section_now == 0, next_in[:, cut], to_next_section(outputs[-1][c]))
                )
                for c, cut in enumerate(cuts)
            ]
            scale = peaks[tick - 1]
        factor = FP8_LIMIT / scale
        dequant = scale / FP8_LIMIT
        gate = up = None
        sent = []
        for c, cut in enumerate(cuts):
            quantized = jnp.clip(
                streams[c].astype(jnp.float32) * factor, -FP8_LIMIT, FP8_LIMIT
            ).astype(jnp.bfloat16)
            if c >= DEPTH:
                quantized = after(quantized, sent[c - DEPTH], first_peak)
            if tick > 0 and c == count - 1:
                seen = [after(s, sent[0]) if sent else s for s in streams]
                here = [jnp.max(jnp.abs(s)).astype(jnp.float32).reshape(1) for s in seen]
                here = jnp.max(jnp.concatenate(here), keepdims=True)
                here = ring_max(ring_max(here, "torus"), "node")
                peaks.append(here[0])
                quantized = after(quantized, here)
            elif tick == 0:
                quantized = after(quantized, known[-1])
            held = [quantized] + [shifted(quantized, "node", -2 * k) for k in range(1, groups)]
            picked = [dot(select[k], held[k]).astype(jnp.bfloat16) for k in range(groups)]
            mine = jnp.concatenate([p[:capacity] for p in picked], axis=0)
            sent.append(jnp.concatenate([p[capacity:] for p in picked], axis=0))
            rows = jnp.concatenate([mine, swapped(sent[c], "node")], axis=0)
            gate_part = dot(rows, gate_mat[cut])
            up_part = dot(rows, up_mat[cut])
            gate = gate_part if gate is None else gate + gate_part
            up = up_part if up is None else up + up_part
        gate = torus_sum(gate) * dequant
        up = torus_sum(up) * dequant
        hidden = (jax.nn.silu(gate) * up).astype(jnp.bfloat16)
        layer, crossed = [], []
        for c, cut in enumerate(cuts):
            away_rows = hidden[half:]
            if c >= DEPTH:
                away_rows = after(away_rows, crossed[c - DEPTH])
            away = dot(away_rows, down_mat[:, cut]).astype(jnp.bfloat16)
            home_rows = after(hidden[:half], away)
            home = dot(home_rows, down_mat[:, cut]).astype(jnp.bfloat16)
            back = swapped(away, "node")
            branch = None
            for k in reversed(range(groups)):
                span = slice(k * capacity, (k + 1) * capacity)
                part = dot(combine[k], jnp.concatenate([home[span], back[span]], axis=0))
                if k > 0:
                    part = part.astype(jnp.bfloat16)
                    crossed = crossed + [part] if k == groups - 1 else crossed
                    part = shifted(part, "node", 2 * k).astype(jnp.float32)
                branch = part if branch is None else branch + part
            layer.append((streams[c].astype(jnp.float32) + branch).astype(jnp.bfloat16))
        outputs.append(layer)
    act_out = jnp.stack([jnp.concatenate(layer, axis=1) for layer in outputs])
    return act_out[:, None], jnp.stack(peaks)[None, :]


def solution(mesh):
    return jax.shard_map(
        shards,
        mesh=mesh,
        in_specs=(
            P("section", "node", "torus"),
            P("node", "torus"),
            P(None, "section", "node", None),
            P(None, "section", "node", None),
            P("section"),
            P("section", "node", "torus", None),
            P("section", "node", "torus", None),
            P("section", "node", None, "torus"),
        ),
        out_specs=(P(None, "section", "node", "torus"), P("section", None)),
        check_vma=False,
    )
```
